32 devices in a mesh: bank: 4 (over z), zero: 8 (over y, x, core).
Axes of the slice: x: 2, y: 2, z: 4, core: 2. Of those that a mesh axis runs over, the one named last changes fastest.
Arguments:
- w_gate: float32 [128, 2048, 768], P('bank', 'zero'), may hold values from -0.1875 to 0.1875
- w_up: float32 [128, 2048, 768], P('bank', 'zero'), may hold values from -0.1875 to 0.1875
- router_weight: float32 [2048, 128], P('zero', 'bank'), may hold values from -0.125 to 0.125
- router_gain: float32 [2048], P('zero'), may hold values from 0.25 to 1.75
Outputs:
- serve_gate: bfloat16 [128, 2048, 768], P('bank', None, 'zero')
- serve_up: bfloat16 [128, 2048, 768], P('bank', None, 'zero')
- scale_gate: float32 [128, 768], P('bank', 'zero')
- scale_up: float32 [128, 768], P('bank', 'zero')
- serve_router: bfloat16 [2048, 128], replicated
The draws below stay inside these ranges and needn't reach their ends.
All inputs are finite; a program needn't handle non-finite values.
Results may differ from the reference program's by a relative error of at most 0.001.
Values may be sent and summed in bfloat16 or wider, within the bound.
A program may use at most 192 MiB of HBM per device.

```python
import jax
import jax.numpy as jnp
from jax import lax

EXPERTS = 128
D_MODEL = 2048
D_EXPERT = 768


def strengthened(drawn, own_key, source, target, shards_of, factor):
    owner, partner = [(jnp.arange(drawn.shape[position]) // (drawn.shape[position] // shards_of)).reshape([-1 if axis == position else 1 for axis in range(drawn.ndim)]) for position in (source, target)]
    chosen = jax.random.permutation(own_key, shards_of)[partner]
    strong = (owner == chosen) | (owner == (partner + shards_of // 2) % shards_of)
    return jnp.where(strong, factor * drawn, drawn)


def block_levels(key, shape, shards, least, top_value):
    gain, own = 1.0, jax.random.fold_in(key, 6)
    for dim, blocks in shards:
        steps = jnp.exp(jax.random.uniform(jax.random.fold_in(own, dim), (blocks,), jnp.float32, least / len(shards), top_value / len(shards)))
        gain = gain * jnp.repeat(steps, shape[dim] // blocks).reshape([-1 if axis == dim else 1 for axis in range(len(shape))])
    return gain


def noise(stream_key, shape, spread, limit, cuts=(), dtype=jnp.bfloat16):
    result = jax.random.normal(stream_key, shape, jnp.float32) * spread
    if len(cuts) > 0:
        result = block_levels(stream_key, shape, cuts, -0.22, 0.18) * result
    return jnp.clip(result, min=-limit, max=limit).astype(dtype)


def bell_draw_with(key, extent, scale, limit, shards, heavy, held_as=jnp.bfloat16):
    drawn = scale * jax.random.normal(key, extent, jnp.float32)
    if shards:
        drawn = drawn * block_levels(key, extent, shards, -0.22, 0.18)
    return jnp.clip(strengthened(drawn, jax.random.fold_in(key, 3), *heavy), -limit, limit).astype(held_as)


def setup_inputs(seed: int = 0) -> dict:
    streams_of = jax.random.split(jax.random.key(seed), 5)
    return {
        "w_gate": bell_draw_with(streams_of[0], (EXPERTS, D_MODEL, D_EXPERT), D_MODEL ** -0.5, 0.1875, ((0, 4), (1, 8)), (1, 2, 8, 2.0), jnp.float32),
        "w_up": bell_draw_with(streams_of[1], (EXPERTS, D_MODEL, D_EXPERT), D_MODEL ** -0.5, 0.1875, ((0, 4), (1, 8)), (1, 2, 8, 2.0), jnp.float32),
        "router_weight": noise(streams_of[2], (D_MODEL, EXPERTS), D_MODEL ** -0.5, 0.125, ((0, 8), (1, 4)), jnp.float32),
        "router_gain": jnp.clip(1.0 + 0.15 * jax.random.normal(streams_of[3], (D_MODEL,), jnp.float32), 0.25, 1.75),
    }


def reference(w_gate, w_up, router_weight, router_gain):
    scale_gate = jnp.sqrt(lax.optimization_barrier(jnp.sum(w_gate * w_gate, axis=1)))
    serve_gate = (w_gate / jnp.expand_dims(scale_gate, 1)).astype(jnp.bfloat16)
    scale_up = jnp.sqrt(lax.optimization_barrier(jnp.sum(w_up * w_up, axis=1)))
    serve_up = (w_up / jnp.expand_dims(scale_up, 1)).astype(jnp.bfloat16)
    serve_router = (router_weight * router_gain[:, None]).astype(jnp.bfloat16)
    return (serve_gate, serve_up, scale_gate, scale_up, serve_router)
```

```python
import functools

import jax
import jax.numpy as jnp
from jax import lax
from jax.experimental import pallas as pl
from jax.experimental.pallas import tpu as pltpu
from jax.sharding import PartitionSpec as P

MESH = pl.DeviceIdType.MESH
AHEAD = 2
VMEM_LIMIT = 32 * 2**20
SLOTS = 8


def flip(index, mask, bits):
    out = 0
    for bit in range(bits):
        here = lax.rem(lax.div(index, 2**bit), 2)
        out = out + (1 - here if (mask >> bit) & 1 else here) * 2**bit
    return out


def exchange_kernel(
    parts,
    banks,
    gate_ref,
    up_ref,
    router_ref,
    gain_ref,
    landing,
    scale_out,
    router_out,
    ring,
    outgoing,
    sums,
    sums_in,
    scales,
    row_router,
    routers,
    load_sem,
    send_sem,
    recv_sem,
    sum_send,
    sum_recv,
    scale_send,
    scale_recv,
    row_send,
    row_recv,
    bank_send,
    bank_recv,
):
    experts, rows, columns = gate_ref.shape
    width = columns // parts
    total = 2 * experts
    batches = total // parts
    depth = ring.shape[0]
    bits = parts.bit_length() - 1
    me, bank = lax.axis_index("zero"), lax.axis_index("bank")
    masks = sorted(range(1, parts), key=lambda m: (m == 1, m % 2, -(m // 2)))
    peers = [flip(me, mask, bits) for mask in masks]
    own_rows = pl.ds(pl.multiple_of(me * rows, 128), rows)

    def remote(src, dst, send, recv, **device):
        return pltpu.make_async_remote_copy(
            src_ref=src,
            dst_ref=dst,
            send_sem=send,
            recv_sem=recv,
            device_id=device,
            device_id_type=MESH,
        )

    def load(e):
        slot = lax.rem(e, depth)

        @pl.when(e < experts)
        def _():
            pltpu.make_async_copy(gate_ref.at[e], ring.at[slot], load_sem.at[slot]).start()

        @pl.when(e >= experts)
        def _():
            pltpu.make_async_copy(
                up_ref.at[e - experts], ring.at[slot], load_sem.at[slot]
            ).start()

    def square(e):
        slot = lax.rem(e, depth)
        pltpu.make_async_copy(gate_ref.at[0], ring.at[slot], load_sem.at[slot]).wait()
        w = ring[slot]
        sums[e] = jnp.sum(w * w, axis=0, keepdims=True)

    def send_sums(b):
        for peer in peers:
            remote(
                sums.at[b * parts + peer],
                sums_in.at[b, me],
                sum_send.at[b],
                sum_recv.at[b],
                zero=peer,
            ).start()

    def others(ref):
        return ref.at[pl.ds(0, parts - 1)]

    def finish_sums(b):
        remote(
            others(sums_in.at[b]), others(sums_in.at[b]), sum_send.at[b], sum_recv.at[b], zero=me
        ).wait_recv()
        sums_in[b, me] = sums[b * parts + me]
        whole = sums_in[b, 0]
        for part in range(1, parts):
            whole = whole + sums_in[b, part]
        scales[b * parts + me] = jnp.sqrt(whole)
        row = scales.at[b * parts + me]
        for peer in peers:
            remote(row, row, scale_send.at[b], scale_recv.at[b], zero=peer).start()

    def wait_scales(b):
        remote(
            others(scales), others(scales), scale_send.at[b], scale_recv.at[b], zero=me
        ).wait_recv()

    def keep_scales(b):
        first = pl.multiple_of(b * parts, 8)
        whole = jnp.concatenate([scales[b * parts + j] for j in range(parts)], axis=0)
        own = jnp.zeros((parts, width), jnp.float32)
        for part in range(parts):
            own = jnp.where(me == part, whole[:, part * width : (part + 1) * width], own)
        scale_out[pl.ds(first, parts), :] = own

    def send_piece(e, slot, at):
        return remote(
            outgoing.at[slot, peers[at]],
            landing.at[e, :, own_rows],
            send_sem.at[slot, at],
            recv_sem.at[me],
            zero=peers[at],
        )

    def row_piece(peer):
        return remote(
            row_router, routers.at[bank, :, own_rows], row_send, row_recv, zero=peer
        )

    def all_rows():
        part = routers.at[bank, :, pl.ds(0, (parts - 1) * rows)]
        return remote(part, part, row_send, row_recv, zero=me)

    def bank_piece(step):
        other = lax.rem(bank + step, banks)
        return remote(
            routers.at[bank], routers.at[bank], bank_send, bank_recv, bank=other
        )

    def all_banks():
        part = routers.at[pl.ds(0, banks - 1)]
        return remote(part, part, bank_send, bank_recv, zero=me)

    lax.fori_loop(0, depth, lambda e, c: (load(e), c)[1], 0)

    barrier = pltpu.get_barrier_semaphore()
    for peer in peers:
        pl.semaphore_signal(barrier, inc=1, device_id={"zero": peer}, device_id_type=MESH)
    for step in range(1, banks):
        pl.semaphore_signal(
            barrier,
            inc=1,
            device_id={"bank": lax.rem(bank + step, banks)},
            device_id_type=MESH,
        )

    lax.fori_loop(0, parts, lambda e, c: (square(e), c)[1], 0)
    pl.semaphore_wait(barrier, parts - 1 + banks - 1)
    send_sums(0)
    part_router = (router_ref[...] * gain_ref[...]).astype(jnp.bfloat16)
    row_router[...] = part_router
    routers[bank, :, own_rows] = part_router
    lax.fori_loop(parts, AHEAD * parts, lambda e, c: (square(e), c)[1], 0)
    finish_sums(0)
    for b in range(1, AHEAD):
        send_sums(b)

    def step(s, carry):
        b, i = lax.div(s, parts), lax.rem(s, parts)
        slot = lax.rem(s, SLOTS)

        @pl.when(i == 0)
        def _():
            wait_scales(b)

        @pl.when(s >= SLOTS)
        def _():
            for at in range(parts - 1):
                send_piece(s, slot, at).wait_send()

        turned = (ring[lax.rem(s, depth)] / scales[s]).T
        for part in range(parts):
            outgoing[slot, part] = turned[part * width : (part + 1) * width].astype(
                jnp.bfloat16
            )
        landing[s, :, own_rows] = outgoing[slot, me]

        @pl.when(s + depth < total)
        def _():
            load(s + depth)

        for at in range(parts - 1):
            send_piece(s, slot, at).start()

        @pl.when(s + AHEAD * parts < total)
        def _():
            square(s + AHEAD * parts)

        @pl.when(jnp.logical_and(i == parts - 1, b + AHEAD < batches))
        def _():
            send_sums(b + AHEAD)

        @pl.when(jnp.logical_and(i == parts // 2, b + 1 < batches))
        def _():
            finish_sums(b + 1)

        @pl.when(i == 2)
        def _():
            keep_scales(b)

        @pl.when(s == 1)
        def _():
            for peer in peers:
                row_piece(peer).start()

        @pl.when(s == total // 4)
        def _():
            all_rows().wait_recv()
            for hop in range(1, banks):
                bank_piece(hop).start()

        return carry

    lax.fori_loop(0, total, step, 0)

    all_banks().wait_send()
    all_banks().wait_recv()
    all_rows().wait_send()
    turned = routers[...].reshape(banks * router_ref.shape[0], parts * rows).T
    router_out[...] = turned

    for b in range(batches):
        for sems, buffer in ((sum_send, sums_in.at[0]), (scale_send, scales)):
            remote(others(buffer), others(buffer), sems.at[b], sems.at[b], zero=me).wait_send()
    for s in range(total - SLOTS, total):
        for at in range(parts - 1):
            send_piece(s, s % SLOTS, at).wait_send()
    for peer in peers:
        region = landing.at[:, :, pl.ds(pl.multiple_of(peer * rows, 128), rows)]
        remote(region, region, recv_sem.at[me], recv_sem.at[peer], zero=me).wait_recv()


def exchange(parts, banks, w_gate, w_up, router_weight, router_gain):
    experts, rows, columns = w_gate.shape
    width = columns // parts
    total = 2 * experts
    batches = total // parts
    held = router_weight.shape[1]
    vmem = pl.BlockSpec(memory_space=pltpu.VMEM)
    hbm = pl.BlockSpec(memory_space=pl.ANY)
    depth = (AHEAD + 1) * parts
    dma = pltpu.SemaphoreType.DMA
    return pl.pallas_call(
        functools.partial(exchange_kernel, parts, banks),
        in_specs=[hbm, hbm, vmem, vmem],
        out_specs=[vmem] * 3,
        out_shape=[
            pltpu.VMEM((total, width, parts * rows), jnp.bfloat16),
            pltpu.VMEM((total, width), jnp.float32),
            pltpu.VMEM((parts * rows, banks * held), jnp.bfloat16),
        ],
        scratch_shapes=[
            pltpu.VMEM((depth, rows, columns), jnp.float32),
            pltpu.VMEM((SLOTS, parts, width, rows), jnp.bfloat16),
            pltpu.VMEM((total, 1, columns), jnp.float32),
            pltpu.VMEM((batches, parts, 1, columns), jnp.float32),
            pltpu.VMEM((total, 1, columns), jnp.float32),
            pltpu.VMEM((held, rows), jnp.bfloat16),
            pltpu.VMEM((banks, held, parts * rows), jnp.bfloat16),
            dma((depth,)),
            dma((SLOTS, parts - 1)),
            dma((parts,)),
            dma((batches,)),
            dma((batches,)),
            dma((batches,)),
            dma((batches,)),
            dma,
            dma,
            dma,
            dma,
        ],
        cost_estimate=pl.CostEstimate(
            flops=total * rows * columns * 60,
            bytes_accessed=total * rows * columns * 4,
            transcendentals=0,
        ),
        compiler_params=pltpu.CompilerParams(
            collective_id=0, has_side_effects=True, vmem_limit_bytes=VMEM_LIMIT
        ),
        name="exchange",
    )(
        pltpu.with_memory_space_constraint(w_gate, pltpu.HBM),
        pltpu.with_memory_space_constraint(w_up, pltpu.HBM),
        router_weight.T,
        router_gain[None, :],
    )


def deliver_kernel(pieces, landing, scales, router, gate, up, scale_gate, scale_up, out, sem):
    experts = gate.shape[0]
    size = experts // pieces
    copies = []
    for which, target in enumerate((gate, up)):
        for piece in range(pieces):
            copies.append(
                (
                    landing.at[pl.ds(which * experts + piece * size, size)],
                    target.at[pl.ds(piece * size, size)],
                )
            )
    copies.append((scales.at[pl.ds(0, experts)], scale_gate))
    copies.append((scales.at[pl.ds(experts, experts)], scale_up))
    copies.append((router, out))
    handles = [
        pltpu.make_async_copy(source, target, sem.at[at])
        for at, (source, target) in enumerate(copies)
    ]
    for handle in handles:
        handle.start()
    for handle in handles:
        handle.wait()


def deliver(landing, scales, router):
    total, width, rows = landing.shape
    experts = total // 2
    pieces = 8 if experts % 8 == 0 else 1
    vmem = pl.BlockSpec(memory_space=pltpu.VMEM)
    hbm = pl.BlockSpec(memory_space=pl.ANY)
    return pl.pallas_call(
        functools.partial(deliver_kernel, pieces),
        in_specs=[vmem] * 3,
        out_specs=[hbm] * 5,
        out_shape=[
            jax.ShapeDtypeStruct((experts, width, rows), landing.dtype),
            jax.ShapeDtypeStruct((experts, width, rows), landing.dtype),
            jax.ShapeDtypeStruct((experts, width), jnp.float32),
            jax.ShapeDtypeStruct((experts, width), jnp.float32),
            jax.ShapeDtypeStruct(router.shape, router.dtype),
        ],
        scratch_shapes=[pltpu.SemaphoreType.DMA((2 * pieces + 3,))],
        cost_estimate=pl.CostEstimate(
            flops=total * rows * width, bytes_accessed=4 * total * rows * width, transcendentals=0
        ),
        compiler_params=pltpu.CompilerParams(vmem_limit_bytes=2**20),
        name="deliver",
    )(*(pltpu.with_memory_space_constraint(x, pltpu.VMEM) for x in (landing, scales, router)))


def shards_blocked(parts, banks, w_gate, w_up, router_weight, router_gain):
    arrived = exchange(parts, banks, w_gate, w_up, router_weight, router_gain)
    gate, up, scale_gate, scale_up, router = deliver(*arrived)
    return gate.transpose(0, 2, 1), up.transpose(0, 2, 1), scale_gate, scale_up, router


def shards_plain(w_gate, w_up, router_weight, router_gain):
    total_gate, total_up = lax.psum(
        (jnp.sum(w_gate * w_gate, axis=1), jnp.sum(w_up * w_up, axis=1)), "zero"
    )
    results, own = [], []
    for w, total in ((w_gate, total_gate), (w_up, total_up)):
        scale = jnp.sqrt(total)
        narrow = (w / jnp.expand_dims(scale, 1)).astype(jnp.bfloat16)
        serve = lax.all_to_all(narrow, "zero", split_axis=2, concat_axis=1, tiled=True)
        width = serve.shape[2]
        results.append(serve)
        own.append(
            lax.dynamic_slice_in_dim(scale, lax.axis_index("zero") * width, width, axis=1)
        )
    part_router = (router_weight * router_gain[:, None]).astype(jnp.bfloat16)
    row_router = lax.all_gather(part_router, "zero", axis=0, tiled=True)
    serve_router = lax.all_gather(row_router, "bank", axis=1, tiled=True)
    return (*results, *own, serve_router)


def solution(mesh):
    parts, banks = mesh.shape["zero"], mesh.shape["bank"]
    placed = (P("bank", "zero", None), P("bank", "zero", None), P("zero", "bank"), P("zero"))

    def shards(w_gate, w_up, router_weight, router_gain):
        experts, rows, columns = w_gate.shape
        held = router_weight.shape[1]
        total = 2 * experts
        power = parts & (parts - 1) == 0 and parts % 8 == 0
        whole = rows % 128 == 0 and columns % (16 * parts) == 0 and held % 16 == 0
        if power and whole and total % parts == 0 and total >= (AHEAD + 1) * parts:
            return shards_blocked(parts, banks, w_gate, w_up, router_weight, router_gain)
        return shards_plain(w_gate, w_up, router_weight, router_gain)

    return jax.shard_map(
        shards,
        mesh=mesh,
        in_specs=placed,
        out_specs=(
            P("bank", None, "zero"),
            P("bank", None, "zero"),
            P("bank", "zero"),
            P("bank", "zero"),
            P(),
        ),
        check_vma=False,
    )
```

```python
import functools

import jax
import jax.numpy as jnp
from jax import lax
from jax.experimental import pallas as pl
from jax.experimental.pallas import tpu as pltpu
from jax.sharding import PartitionSpec as P

MESH = pl.DeviceIdType.MESH
FIRST = 2
LOADS = 4
VMEM_LIMIT = 32 * 2**20
SLOTS = 8


def flip(index, mask, bits):
    out = 0
    for bit in range(bits):
        here = lax.rem(lax.div(index, 2**bit), 2)
        out = out + (1 - here if (mask >> bit) & 1 else here) * 2**bit
    return out


def exchange_kernel(
    parts,
    banks,
    gate_ref,
    up_ref,
    router_ref,
    gain_ref,
    landing,
    scale_out,
    router_out,
    ring,
    outgoing,
    first_in,
    sums,
    pair_in,
    chip_sums,
    chip_in,
    scales,
    row_router,
    routers,
    load_sem,
    send_sem,
    recv_sem,
    first_send,
    first_recv,
    batch_send,
    batch_recv,
    row_send,
    row_recv,
    bank_send,
    bank_recv,
):
    experts, rows, columns = gate_ref.shape
    width = columns // parts
    total = 2 * experts
    batches = total // parts
    half = parts // 2
    depth = ring.shape[0]
    bits = parts.bit_length() - 1
    me, bank = lax.axis_index("zero"), lax.axis_index("bank")
    side, place = lax.rem(me, 2), lax.div(me, 2)
    masks = sorted(range(1, parts), key=lambda m: (m == 1, m % 2, -(m // 2)))
    peers = [flip(me, mask, bits) for mask in masks]
    partner = flip(me, 1, bits)
    cohort = [flip(me, mask, bits) for mask in masks if mask % 2 == 0]
    own_rows = pl.ds(pl.multiple_of(me * rows, 128), rows)

    def remote(src, dst, send, recv, **device):
        return pltpu.make_async_remote_copy(
            src_ref=src,
            dst_ref=dst,
            send_sem=send,
            recv_sem=recv,
            device_id=device,
            device_id_type=MESH,
        )

    def load(e):
        slot = lax.rem(e, depth)

        @pl.when(e < experts)
        def _():
            pltpu.make_async_copy(gate_ref.at[e], ring.at[slot], load_sem.at[slot]).start()

        @pl.when(e >= experts)
        def _():
            pltpu.make_async_copy(
                up_ref.at[e - experts], ring.at[slot], load_sem.at[slot]
            ).start()

    def square(e):
        slot = lax.rem(e, depth)
        pltpu.make_async_copy(gate_ref.at[0], ring.at[slot], load_sem.at[slot]).wait()
        w = ring[slot]
        return jnp.sum(w * w, axis=0, keepdims=True)

    def where_of(e):
        i = lax.rem(e, parts)
        return lax.div(e, parts), lax.rem(i, 2), lax.div(i, 2)

    def first_square(e, carry):
        first_in[me, e] = square(e)
        load(e + LOADS)
        return carry

    def later_square(e, carry):
        sums[where_of(e)] = square(e)
        return carry

    groups = ((0, FIRST), (FIRST, parts - FIRST))

    def send_first(group):
        part = first_in.at[me, pl.ds(*groups[group])]
        for peer in peers:
            remote(part, part, first_send.at[group], first_recv.at[group], zero=peer).start()

    def all_first(group):
        part = first_in.at[pl.ds(0, parts - 1), pl.ds(*groups[group])]
        return remote(part, part, first_send.at[group], first_recv.at[group], zero=me)

    def finish_first(group):
        all_first(group).wait_recv()
        for e in range(groups[group][0], sum(groups[group])):
            whole = first_in[0, e]
            for part in range(1, parts):
                whole = whole + first_in[part, e]
            scales[0, e % 2, e // 2] = jnp.sqrt(whole)

    def pair_sums(b):
        return remote(
            sums.at[b, 1 - side],
            pair_in.at[b],
            batch_send.at[0, b],
            batch_recv.at[0, b],
            zero=partner,
        )

    def chip_piece(b, peer):
        return remote(
            chip_sums.at[b, lax.div(peer, 2)],
            chip_in.at[b, place],
            batch_send.at[1, b],
            batch_recv.at[1, b],
            zero=peer,
        )

    def scale_piece(b, peer):
        row = scales.at[b, side, place]
        return remote(row, row, batch_send.at[2, b], batch_recv.at[2, b], zero=peer)

    def pair_scales(b):
        mine = scales.at[b, side]
        return remote(mine, mine, batch_send.at[3, b], batch_recv.at[3, b], zero=partner)

    def all_pieces(stage, b):
        part = chip_in.at[b, pl.ds(0, half - 1)]
        return remote(part, part, batch_send.at[stage, b], batch_recv.at[stage, b], zero=me)

    def stage_chip(b):
        pair_sums(b).wait_recv()
        for q in range(half):
            chip_sums[b, q] = pair_in[b, q] + sums[b, side, q]
        chip_in[b, place] = chip_sums[b, place]
        for peer in cohort:
            chip_piece(b, peer).start()

    def stage_scale(b):
        all_pieces(1, b).wait_recv()
        whole = chip_in[b, 0]
        for q in range(1, half):
            whole = whole + chip_in[b, q]
        scales[b, side, place] = jnp.sqrt(whole)
        for peer in cohort:
            scale_piece(b, peer).start()

    def stage_share(b):
        all_pieces(2, b).wait_recv()
        pair_scales(b).start()

    def keep_scales(b):
        start = pl.multiple_of(b * parts, 8)
        whole = jnp.concatenate([scales[b, j % 2, j // 2] for j in range(parts)], axis=0)
        own = jnp.zeros((parts, width), jnp.float32)
        for part in range(parts):
            own = jnp.where(me == part, whole[:, part * width : (part + 1) * width], own)
        scale_out[pl.ds(start, parts), :] = own

    def send_piece(e, slot, at):
        return remote(
            outgoing.at[slot, peers[at]],
            landing.at[e, :, own_rows],
            send_sem.at[slot, at],
            recv_sem.at[me],
            zero=peers[at],
        )

    def row_piece(peer):
        return remote(
            row_router, routers.at[bank, :, own_rows], row_send, row_recv, zero=peer
        )

    def all_rows():
        part = routers.at[bank, :, pl.ds(0, (parts - 1) * rows)]
        return remote(part, part, row_send, row_recv, zero=me)

    def bank_piece(step):
        other = lax.rem(bank + step, banks)
        return remote(
            routers.at[bank], routers.at[bank], bank_send, bank_recv, bank=other
        )

    def all_banks():
        part = routers.at[pl.ds(0, banks - 1)]
        return remote(part, part, bank_send, bank_recv, zero=me)

    for e in range(LOADS):
        load(jnp.int32(e))

    barrier = pltpu.get_barrier_semaphore()
    for peer in peers:
        pl.semaphore_signal(barrier, inc=1, device_id={"zero": peer}, device_id_type=MESH)
    for step in range(1, banks):
        pl.semaphore_signal(
            barrier,
            inc=1,
            device_id={"bank": lax.rem(bank + step, banks)},
            device_id_type=MESH,
        )

    part_router = (router_ref[...] * gain_ref[...]).astype(jnp.bfloat16)
    row_router[...] = part_router
    routers[bank, :, own_rows] = part_router
    lax.fori_loop(0, FIRST, first_square, 0)
    pl.semaphore_wait(barrier, parts - 1 + banks - 1)
    send_first(0)
    for peer in peers:
        row_piece(peer).start()
    lax.fori_loop(FIRST, parts, first_square, 0)
    send_first(1)
    finish_first(0)

    def step(s, carry):
        b, i = lax.div(s, parts), lax.rem(s, parts)
        slot = lax.rem(s, SLOTS)

        @pl.when(jnp.logical_and(i == 0, b > 0))
        def _():
            pair_scales(b).wait_recv()

        @pl.when(s >= SLOTS)
        def _():
            for at in range(parts - 1):
                send_piece(s, slot, at).wait_send()

        turned = (ring[lax.rem(s, depth)] / scales[where_of(s)]).T
        for part in range(parts):
            outgoing[slot, part] = turned[part * width : (part + 1) * width].astype(
                jnp.bfloat16
            )
        landing[s, :, own_rows] = outgoing[slot, me]

        @pl.when(s + 2 * parts + LOADS < total)
        def _():
            load(s + 2 * parts + LOADS)

        for at in range(parts - 1):
            send_piece(s, slot, at).start()

        @pl.when(s == 0)
        def _():
            def ahead(e, carry):
                load(e + LOADS)
                return later_square(e, carry)

            lax.fori_loop(parts, 2 * parts, ahead, 0)
            pair_sums(1).start()

        @pl.when(s == 1)
        def _():
            finish_first(1)

        @pl.when(s + 2 * parts < total)
        def _():
            later_square(s + 2 * parts, 0)

        @pl.when(jnp.logical_and(i == parts - 1, b + 2 < batches))
        def _():
            pair_sums(b + 2).start()

        @pl.when(b + 1 < batches)
        def _():
            @pl.when(i == 1)
            def _():
                stage_chip(b + 1)

            @pl.when(i == 3)
            def _():
                stage_scale(b + 1)

            @pl.when(i == 5)
            def _():
                stage_share(b + 1)

        @pl.when(i == 2)
        def _():
            keep_scales(b)

        @pl.when(s == parts)
        def _():
            all_rows().wait_recv()
            for hop in range(1, banks):
                bank_piece(hop).start()

        return carry

    lax.fori_loop(0, total, step, 0)

    all_banks().wait_send()
    all_banks().wait_recv()
    all_rows().wait_send()
    turned = routers[...].reshape(banks * router_ref.shape[0], parts * rows).T
    router_out[...] = turned

    for group in range(2):
        all_first(group).wait_send()
    for b in range(1, batches):
        pair_sums(b).wait_send()
        all_pieces(1, b).wait_send()
        all_pieces(2, b).wait_send()
        pair_scales(b).wait_send()
    for s in range(total - SLOTS, total):
        for at in range(parts - 1):
            send_piece(s, s % SLOTS, at).wait_send()
    for peer in peers:
        region = landing.at[:, :, pl.ds(pl.multiple_of(peer * rows, 128), rows)]
        remote(region, region, recv_sem.at[me], recv_sem.at[peer], zero=me).wait_recv()


def exchange(parts, banks, w_gate, w_up, router_weight, router_gain):
    experts, rows, columns = w_gate.shape
    width = columns // parts
    total = 2 * experts
    batches = total // parts
    held = router_weight.shape[1]
    vmem = pl.BlockSpec(memory_space=pltpu.VMEM)
    hbm = pl.BlockSpec(memory_space=pl.ANY)
    depth = 3 * parts
    half = parts // 2
    row = (1, columns)
    dma = pltpu.SemaphoreType.DMA
    return pl.pallas_call(
        functools.partial(exchange_kernel, parts, banks),
        in_specs=[hbm, hbm, vmem, vmem],
        out_specs=[vmem] * 3,
        out_shape=[
            pltpu.VMEM((total, width, parts * rows), jnp.bfloat16),
            pltpu.VMEM((total, width), jnp.float32),
            pltpu.VMEM((parts * rows, banks * held), jnp.bfloat16),
        ],
        scratch_shapes=[
            pltpu.VMEM((depth, rows, columns), jnp.float32),
            pltpu.VMEM((SLOTS, parts, width, rows), jnp.bfloat16),
            pltpu.VMEM((parts, parts) + row, jnp.float32),
            pltpu.VMEM((batches, 2, half) + row, jnp.float32),
            pltpu.VMEM((batches, half) + row, jnp.float32),
            pltpu.VMEM((batches, half) + row, jnp.float32),
            pltpu.VMEM((batches, half) + row, jnp.float32),
            pltpu.VMEM((batches, 2, half) + row, jnp.float32),
            pltpu.VMEM((held, rows), jnp.bfloat16),
            pltpu.VMEM((banks, held, parts * rows), jnp.bfloat16),
            dma((depth,)),
            dma((SLOTS, parts - 1)),
            dma((parts,)),
            dma((2,)),
            dma((2,)),
            dma((4, batches)),
            dma((4, batches)),
            dma,
            dma,
            dma,
            dma,
        ],
        cost_estimate=pl.CostEstimate(
            flops=total * rows * columns * 60,
            bytes_accessed=total * rows * columns * 4,
            transcendentals=0,
        ),
        compiler_params=pltpu.CompilerParams(
            collective_id=0, has_side_effects=True, vmem_limit_bytes=VMEM_LIMIT
        ),
        name="exchange",
    )(
        pltpu.with_memory_space_constraint(w_gate, pltpu.HBM),
        pltpu.with_memory_space_constraint(w_up, pltpu.HBM),
        router_weight.T,
        router_gain[None, :],
    )


def deliver_kernel(pieces, landing, scales, router, gate, up, scale_gate, scale_up, out, sem):
    experts = gate.shape[0]
    size = experts // pieces
    copies = []
    for which, target in enumerate((gate, up)):
        for piece in range(pieces):
            copies.append(
                (
                    landing.at[pl.ds(which * experts + piece * size, size)],
                    target.at[pl.ds(piece * size, size)],
                )
            )
    copies.append((scales.at[pl.ds(0, experts)], scale_gate))
    copies.append((scales.at[pl.ds(experts, experts)], scale_up))
    copies.append((router, out))
    handles = [
        pltpu.make_async_copy(source, target, sem.at[at])
        for at, (source, target) in enumerate(copies)
    ]
    for handle in handles:
        handle.start()
    for handle in handles:
        handle.wait()


def deliver(landing, scales, router):
    total, width, rows = landing.shape
    experts = total // 2
    pieces = 8 if experts % 8 == 0 else 1
    vmem = pl.BlockSpec(memory_space=pltpu.VMEM)
    hbm = pl.BlockSpec(memory_space=pl.ANY)
    return pl.pallas_call(
        functools.partial(deliver_kernel, pieces),
        in_specs=[vmem] * 3,
        out_specs=[hbm] * 5,
        out_shape=[
            jax.ShapeDtypeStruct((experts, width, rows), landing.dtype),
            jax.ShapeDtypeStruct((experts, width, rows), landing.dtype),
            jax.ShapeDtypeStruct((experts, width), jnp.float32),
            jax.ShapeDtypeStruct((experts, width), jnp.float32),
            jax.ShapeDtypeStruct(router.shape, router.dtype),
        ],
        scratch_shapes=[pltpu.SemaphoreType.DMA((2 * pieces + 3,))],
        cost_estimate=pl.CostEstimate(
            flops=total * rows * width, bytes_accessed=4 * total * rows * width, transcendentals=0
        ),
        compiler_params=pltpu.CompilerParams(vmem_limit_bytes=2**20),
        name="deliver",
    )(*(pltpu.with_memory_space_constraint(x, pltpu.VMEM) for x in (landing, scales, router)))


def shards_blocked(parts, banks, w_gate, w_up, router_weight, router_gain):
    arrived = exchange(parts, banks, w_gate, w_up, router_weight, router_gain)
    gate, up, scale_gate, scale_up, router = deliver(*arrived)
    return gate.transpose(0, 2, 1), up.transpose(0, 2, 1), scale_gate, scale_up, router


def shards_plain(w_gate, w_up, router_weight, router_gain):
    total_gate, total_up = lax.psum(
        (jnp.sum(w_gate * w_gate, axis=1), jnp.sum(w_up * w_up, axis=1)), "zero"
    )
    results, own = [], []
    for w, total in ((w_gate, total_gate), (w_up, total_up)):
        scale = jnp.sqrt(total)
        narrow = (w / jnp.expand_dims(scale, 1)).astype(jnp.bfloat16)
        serve = lax.all_to_all(narrow, "zero", split_axis=2, concat_axis=1, tiled=True)
        width = serve.shape[2]
        results.append(serve)
        own.append(
            lax.dynamic_slice_in_dim(scale, lax.axis_index("zero") * width, width, axis=1)
        )
    part_router = (router_weight * router_gain[:, None]).astype(jnp.bfloat16)
    row_router = lax.all_gather(part_router, "zero", axis=0, tiled=True)
    serve_router = lax.all_gather(row_router, "bank", axis=1, tiled=True)
    return (*results, *own, serve_router)


def solution(mesh):
    parts, banks = mesh.shape["zero"], mesh.shape["bank"]
    placed = (P("bank", "zero", None), P("bank", "zero", None), P("zero", "bank"), P("zero"))

    def shards(w_gate, w_up, router_weight, router_gain):
        experts, rows, columns = w_gate.shape
        held = router_weight.shape[1]
        total = 2 * experts
        power = parts & (parts - 1) == 0 and parts % 8 == 0
        whole = rows % 128 == 0 and columns % (16 * parts) == 0 and held % 16 == 0
        if power and whole and total % parts == 0 and total >= 3 * parts:
            return shards_blocked(parts, banks, w_gate, w_up, router_weight, router_gain)
        return shards_plain(w_gate, w_up, router_weight, router_gain)

    return jax.shard_map(
        shards,
        mesh=mesh,
        in_specs=placed,
        out_specs=(
            P("bank", None, "zero"),
            P("bank", None, "zero"),
            P("bank", "zero"),
            P("bank", "zero"),
            P(),
        ),
        check_vma=False,
    )
```

```python
import functools

import jax
import jax.numpy as jnp
from jax import lax
from jax.experimental import pallas as pl
from jax.experimental.pallas import tpu as pltpu
from jax.sharding import PartitionSpec as P

MESH = pl.DeviceIdType.MESH
FIRST = 2
LOADS = 4
VMEM_LIMIT = 32 * 2**20
SLOTS = 8


def flip(index, mask, bits):
    out = 0
    for bit in range(bits):
        here = lax.rem(lax.div(index, 2**bit), 2)
        out = out + (1 - here if (mask >> bit) & 1 else here) * 2**bit
    return out


def exchange_kernel(
    parts,
    banks,
    gate_ref,
    up_ref,
    router_ref,
    gain_ref,
    landing,
    scale_out,
    router_out,
    ring,
    outgoing,
    first_in,
    sums,
    pair_in,
    chip_sums,
    chip_in,
    scales,
    row_router,
    routers,
    load_sem,
    send_sem,
    recv_sem,
    first_send,
    first_recv,
    batch_send,
    batch_recv,
    row_send,
    row_recv,
    bank_send,
    bank_recv,
):
    experts, rows, columns = gate_ref.shape
    width = columns // parts
    total = 2 * experts
    batches = total // parts
    half = parts // 2
    depth = ring.shape[0]
    bits = parts.bit_length() - 1
    me, bank = lax.axis_index("zero"), lax.axis_index("bank")
    side, place = lax.rem(me, 2), lax.div(me, 2)
    masks = sorted(range(1, parts), key=lambda m: (m == 1, m % 2, -(m // 2)))
    peers = [flip(me, mask, bits) for mask in masks]
    partner = flip(me, 1, bits)
    cohort = [flip(me, mask, bits) for mask in masks if mask % 2 == 0]
    own_rows = pl.ds(pl.multiple_of(me * rows, 128), rows)

    def remote(src, dst, send, recv, **device):
        return pltpu.make_async_remote_copy(
            src_ref=src,
            dst_ref=dst,
            send_sem=send,
            recv_sem=recv,
            device_id=device,
            device_id_type=MESH,
        )

    def load(e):
        slot = lax.rem(e, depth)

        @pl.when(e < experts)
        def _():
            pltpu.make_async_copy(gate_ref.at[e], ring.at[slot], load_sem.at[slot]).start()

        @pl.when(e >= experts)
        def _():
            pltpu.make_async_copy(
                up_ref.at[e - experts], ring.at[slot], load_sem.at[slot]
            ).start()

    def square(e):
        slot = lax.rem(e, depth)
        pltpu.make_async_copy(gate_ref.at[0], ring.at[slot], load_sem.at[slot]).wait()
        w = ring[slot]
        return jnp.sum(w * w, axis=0, keepdims=True)

    def where_of(e):
        i = lax.rem(e, parts)
        return lax.div(e, parts), lax.rem(i, 2), lax.div(i, 2)

    def first_square(e, carry):
        first_in[me, e] = square(e)
        load(e + LOADS)
        return carry

    def later_square(e, carry):
        sums[where_of(e)] = square(e)
        return carry

    groups = ((0, FIRST), (FIRST, parts - FIRST))

    def send_first(group):
        part = first_in.at[me, pl.ds(*groups[group])]
        for peer in peers:
            remote(part, part, first_send.at[group], first_recv.at[group], zero=peer).start()

    def all_first(group):
        part = first_in.at[pl.ds(0, parts - 1), pl.ds(*groups[group])]
        return remote(part, part, first_send.at[group], first_recv.at[group], zero=me)

    def finish_first(group):
        all_first(group).wait_recv()
        for e in range(groups[group][0], sum(groups[group])):
            whole = first_in[0, e]
            for part in range(1, parts):
                whole = whole + first_in[part, e]
            scales[0, e % 2, e // 2] = jnp.sqrt(whole)

    def pair_sums(b):
        return remote(
            sums.at[b, 1 - side],
            pair_in.at[b],
            batch_send.at[0, b],
            batch_recv.at[0, b],
            zero=partner,
        )

    def chip_piece(b, peer):
        return remote(
            chip_sums.at[b, lax.div(peer, 2)],
            chip_in.at[b, place],
            batch_send.at[1, b],
            batch_recv.at[1, b],
            zero=peer,
        )

    def scale_piece(b, peer):
        row = scales.at[b, side, place]
        return remote(row, row, batch_send.at[2, b], batch_recv.at[2, b], zero=peer)

    def pair_scales(b):
        mine = scales.at[b, side]
        return remote(mine, mine, batch_send.at[3, b], batch_recv.at[3, b], zero=partner)

    def all_pieces(stage, b):
        part = chip_in.at[b, pl.ds(0, half - 1)]
        return remote(part, part, batch_send.at[stage, b], batch_recv.at[stage, b], zero=me)

    def stage_chip(b):
        pair_sums(b).wait_recv()
        for q in range(half):
            chip_sums[b, q] = pair_in[b, q] + sums[b, side, q]
        chip_in[b, place] = chip_sums[b, place]
        for peer in cohort:
            chip_piece(b, peer).start()

    def stage_scale(b):
        all_pieces(1, b).wait_recv()
        whole = chip_in[b, 0]
        for q in range(1, half):
            whole = whole + chip_in[b, q]
        scales[b, side, place] = jnp.sqrt(whole)
        for peer in cohort:
            scale_piece(b, peer).start()

    def stage_share(b):
        all_pieces(2, b).wait_recv()
        pair_scales(b).start()

    def keep_scales(b):
        start = pl.multiple_of(b * parts, 8)
        whole = jnp.concatenate([scales[b, j % 2, j // 2] for j in range(parts)], axis=0)
        own = jnp.zeros((parts, width), jnp.float32)
        for part in range(parts):
            own = jnp.where(me == part, whole[:, part * width : (part + 1) * width], own)
        scale_out[pl.ds(start, parts), :] = own

    def send_piece(e, slot, at):
        return remote(
            outgoing.at[slot, peers[at]],
            landing.at[e, :, own_rows],
            send_sem.at[slot, at],
            recv_sem.at[me],
            zero=peers[at],
        )

    def row_piece(peer):
        return remote(
            row_router, routers.at[bank, :, own_rows], row_send, row_recv, zero=peer
        )

    def all_rows():
        part = routers.at[bank, :, pl.ds(0, (parts - 1) * rows)]
        return remote(part, part, row_send, row_recv, zero=me)

    def line(hop, send):
        for way, turn in enumerate((1, -1)):
            source = bank - turn * (hop - 1 if send else hop)
            target = bank + turn
            fits = jnp.logical_and(source >= 0, source < banks)
            if send:
                fits = fits & jnp.logical_and(target >= 0, target < banks)
            yield fits, source, target, (way, hop)

    def line_copy(source, target, at):
        part = routers.at[source]
        return remote(part, part, bank_send.at[at], bank_recv.at[at], bank=target)

    def line_start(hop):
        for fits, source, target, at in line(hop, True):

            @pl.when(fits)
            def _():
                line_copy(source, target, at).start()

    def line_arrived(hop):
        for fits, source, target, at in line(hop, False):

            @pl.when(fits)
            def _():
                line_copy(source, bank, at).wait_recv()

    def line_left(hop):
        for fits, source, target, at in line(hop, True):

            @pl.when(fits)
            def _():
                line_copy(source, target, at).wait_send()

    for e in range(LOADS):
        load(jnp.int32(e))

    barrier = pltpu.get_barrier_semaphore()
    for peer in peers:
        pl.semaphore_signal(barrier, inc=1, device_id={"zero": peer}, device_id_type=MESH)
    around = jnp.int32(0)
    for other in (bank - 1, bank + 1):
        fits = jnp.logical_and(other >= 0, other < banks)
        around = around + jnp.where(fits, 1, 0)

        @pl.when(fits)
        def _():
            pl.semaphore_signal(
                barrier, inc=1, device_id={"bank": other}, device_id_type=MESH
            )

    part_router = (router_ref[...] * gain_ref[...]).astype(jnp.bfloat16)
    row_router[...] = part_router
    routers[bank, :, own_rows] = part_router
    lax.fori_loop(0, FIRST, first_square, 0)
    pl.semaphore_wait(barrier, parts - 1 + around)
    send_first(0)
    for peer in peers:
        row_piece(peer).start()
    lax.fori_loop(FIRST, parts, first_square, 0)
    send_first(1)
    finish_first(0)

    def step(s, carry):
        b, i = lax.div(s, parts), lax.rem(s, parts)
        slot = lax.rem(s, SLOTS)

        @pl.when(jnp.logical_and(i == 0, b > 0))
        def _():
            pair_scales(b).wait_recv()

        @pl.when(s >= SLOTS)
        def _():
            for at in range(parts - 1):
                send_piece(s, slot, at).wait_send()

        turned = (ring[lax.rem(s, depth)] / scales[where_of(s)]).T
        for part in range(parts):
            outgoing[slot, part] = turned[part * width : (part + 1) * width].astype(
                jnp.bfloat16
            )
        landing[s, :, own_rows] = outgoing[slot, me]

        @pl.when(s + 2 * parts + LOADS < total)
        def _():
            load(s + 2 * parts + LOADS)

        for at in range(parts - 1):
            send_piece(s, slot, at).start()

        @pl.when(s == 0)
        def _():
            def ahead(e, carry):
                load(e + LOADS)
                return later_square(e, carry)

            lax.fori_loop(parts, 2 * parts, ahead, 0)
            pair_sums(1).start()

        @pl.when(s == 1)
        def _():
            finish_first(1)

        @pl.when(s + 2 * parts < total)
        def _():
            later_square(s + 2 * parts, 0)

        @pl.when(jnp.logical_and(i == parts - 1, b + 2 < batches))
        def _():
            pair_sums(b + 2).start()

        @pl.when(b + 1 < batches)
        def _():
            @pl.when(i == 1)
            def _():
                stage_chip(b + 1)

            @pl.when(i == 3)
            def _():
                stage_scale(b + 1)

            @pl.when(i == 5)
            def _():
                stage_share(b + 1)

        @pl.when(i == 2)
        def _():
            keep_scales(b)

        for hop in range(1, banks):

            @pl.when(s == hop * parts)
            def _():
                if hop == 1:
                    all_rows().wait_recv()
                else:
                    line_arrived(hop - 1)
                line_start(hop)

        return carry

    lax.fori_loop(0, total, step, 0)

    line_arrived(banks - 1)
    for hop in range(1, banks):
        line_left(hop)
    all_rows().wait_send()
    turned = routers[...].reshape(banks * router_ref.shape[0], parts * rows).T
    router_out[...] = turned

    for group in range(2):
        all_first(group).wait_send()
    for b in range(1, batches):
        pair_sums(b).wait_send()
        all_pieces(1, b).wait_send()
        all_pieces(2, b).wait_send()
        pair_scales(b).wait_send()
    for s in range(total - SLOTS, total):
        for at in range(parts - 1):
            send_piece(s, s % SLOTS, at).wait_send()
    for peer in peers:
        region = landing.at[:, :, pl.ds(pl.multiple_of(peer * rows, 128), rows)]
        remote(region, region, recv_sem.at[me], recv_sem.at[peer], zero=me).wait_recv()


def exchange(parts, banks, w_gate, w_up, router_weight, router_gain):
    experts, rows, columns = w_gate.shape
    width = columns // parts
    total = 2 * experts
    batches = total // parts
    held = router_weight.shape[1]
    vmem = pl.BlockSpec(memory_space=pltpu.VMEM)
    hbm = pl.BlockSpec(memory_space=pl.ANY)
    depth = 3 * parts
    half = parts // 2
    row = (1, columns)
    dma = pltpu.SemaphoreType.DMA
    return pl.pallas_call(
        functools.partial(exchange_kernel, parts, banks),
        in_specs=[hbm, hbm, vmem, vmem],
        out_specs=[vmem] * 3,
        out_shape=[
            pltpu.VMEM((total, width, parts * rows), jnp.bfloat16),
            pltpu.VMEM((total, width), jnp.float32),
            pltpu.VMEM((parts * rows, banks * held), jnp.bfloat16),
        ],
        scratch_shapes=[
            pltpu.VMEM((depth, rows, columns), jnp.float32),
            pltpu.VMEM((SLOTS, parts, width, rows), jnp.bfloat16),
            pltpu.VMEM((parts, parts) + row, jnp.float32),
            pltpu.VMEM((batches, 2, half) + row, jnp.float32),
            pltpu.VMEM((batches, half) + row, jnp.float32),
            pltpu.VMEM((batches, half) + row, jnp.float32),
            pltpu.VMEM((batches, half) + row, jnp.float32),
            pltpu.VMEM((batches, 2, half) + row, jnp.float32),
            pltpu.VMEM((held, rows), jnp.bfloat16),
            pltpu.VMEM((banks, held, parts * rows), jnp.bfloat16),
            dma((depth,)),
            dma((SLOTS, parts - 1)),
            dma((parts,)),
            dma((2,)),
            dma((2,)),
            dma((4, batches)),
            dma((4, batches)),
            dma,
            dma,
            dma((2, banks)),
            dma((2, banks)),
        ],
        cost_estimate=pl.CostEstimate(
            flops=total * rows * columns * 60,
            bytes_accessed=total * rows * columns * 4,
            transcendentals=0,
        ),
        compiler_params=pltpu.CompilerParams(
            collective_id=0, has_side_effects=True, vmem_limit_bytes=VMEM_LIMIT
        ),
        name="exchange",
    )(
        pltpu.with_memory_space_constraint(w_gate, pltpu.HBM),
        pltpu.with_memory_space_constraint(w_up, pltpu.HBM),
        router_weight.T,
        router_gain[None, :],
    )


def deliver_kernel(pieces, landing, scales, router, gate, up, scale_gate, scale_up, out, sem):
    experts = gate.shape[0]
    size = experts // pieces
    copies = []
    for which, target in enumerate((gate, up)):
        for piece in range(pieces):
            copies.append(
                (
                    landing.at[pl.ds(which * experts + piece * size, size)],
                    target.at[pl.ds(piece * size, size)],
                )
            )
    copies.append((scales.at[pl.ds(0, experts)], scale_gate))
    copies.append((scales.at[pl.ds(experts, experts)], scale_up))
    copies.append((router, out))
    handles = [
        pltpu.make_async_copy(source, target, sem.at[at])
        for at, (source, target) in enumerate(copies)
    ]
    for handle in handles:
        handle.start()
    for handle in handles:
        handle.wait()


def deliver(landing, scales, router):
    total, width, rows = landing.shape
    experts = total // 2
    pieces = 8 if experts % 8 == 0 else 1
    vmem = pl.BlockSpec(memory_space=pltpu.VMEM)
    hbm = pl.BlockSpec(memory_space=pl.ANY)
    return pl.pallas_call(
        functools.partial(deliver_kernel, pieces),
        in_specs=[vmem] * 3,
        out_specs=[hbm] * 5,
        out_shape=[
            jax.ShapeDtypeStruct((experts, width, rows), landing.dtype),
            jax.ShapeDtypeStruct((experts, width, rows), landing.dtype),
            jax.ShapeDtypeStruct((experts, width), jnp.float32),
            jax.ShapeDtypeStruct((experts, width), jnp.float32),
            jax.ShapeDtypeStruct(router.shape, router.dtype),
        ],
        scratch_shapes=[pltpu.SemaphoreType.DMA((2 * pieces + 3,))],
        cost_estimate=pl.CostEstimate(
            flops=total * rows * width, bytes_accessed=4 * total * rows * width, transcendentals=0
        ),
        compiler_params=pltpu.CompilerParams(vmem_limit_bytes=2**20),
        name="deliver",
    )(*(pltpu.with_memory_space_constraint(x, pltpu.VMEM) for x in (landing, scales, router)))


def shards_blocked(parts, banks, w_gate, w_up, router_weight, router_gain):
    arrived = exchange(parts, banks, w_gate, w_up, router_weight, router_gain)
    gate, up, scale_gate, scale_up, router = deliver(*arrived)
    return gate.transpose(0, 2, 1), up.transpose(0, 2, 1), scale_gate, scale_up, router


def shards_plain(w_gate, w_up, router_weight, router_gain):
    total_gate, total_up = lax.psum(
        (jnp.sum(w_gate * w_gate, axis=1), jnp.sum(w_up * w_up, axis=1)), "zero"
    )
    results, own = [], []
    for w, total in ((w_gate, total_gate), (w_up, total_up)):
        scale = jnp.sqrt(total)
        narrow = (w / jnp.expand_dims(scale, 1)).astype(jnp.bfloat16)
        serve = lax.all_to_all(narrow, "zero", split_axis=2, concat_axis=1, tiled=True)
        width = serve.shape[2]
        results.append(serve)
        own.append(
            lax.dynamic_slice_in_dim(scale, lax.axis_index("zero") * width, width, axis=1)
        )
    part_router = (router_weight * router_gain[:, None]).astype(jnp.bfloat16)
    row_router = lax.all_gather(part_router, "zero", axis=0, tiled=True)
    serve_router = lax.all_gather(row_router, "bank", axis=1, tiled=True)
    return (*results, *own, serve_router)


def solution(mesh):
    parts, banks = mesh.shape["zero"], mesh.shape["bank"]
    placed = (P("bank", "zero", None), P("bank", "zero", None), P("zero", "bank"), P("zero"))

    def shards(w_gate, w_up, router_weight, router_gain):
        experts, rows, columns = w_gate.shape
        held = router_weight.shape[1]
        total = 2 * experts
        power = parts & (parts - 1) == 0 and parts % 8 == 0
        whole = rows % 128 == 0 and columns % (16 * parts) == 0 and held % 16 == 0
        if power and whole and total % parts == 0 and total >= max(3, banks) * parts:
            return shards_blocked(parts, banks, w_gate, w_up, router_weight, router_gain)
        return shards_plain(w_gate, w_up, router_weight, router_gain)

    return jax.shard_map(
        shards,
        mesh=mesh,
        in_specs=placed,
        out_specs=(
            P("bank", None, "zero"),
            P("bank", None, "zero"),
            P("bank", "zero"),
            P("bank", "zero"),
            P(),
        ),
        check_vma=False,
    )
```

```python
import functools

import jax
import jax.numpy as jnp
from jax import lax
from jax.experimental import pallas as pl
from jax.experimental.pallas import tpu as pltpu
from jax.sharding import PartitionSpec as P

MESH = pl.DeviceIdType.MESH
LATE = 3
FIRST = 2
LOADS = 4
VMEM_LIMIT = 32 * 2**20
SLOTS = 8


def flip(index, mask, bits):
    out = 0
    for bit in range(bits):
        here = lax.rem(lax.div(index, 2**bit), 2)
        out = out + (1 - here if (mask >> bit) & 1 else here) * 2**bit
    return out


def exchange_kernel(
    parts,
    banks,
    gate_ref,
    up_ref,
    router_ref,
    gain_ref,
    landing,
    scale_out,
    router_out,
    *refs,
):
    late = refs[:parts]
    (
        ring,
        outgoing,
        first_in,
        sums,
        pair_in,
        chip_sums,
        chip_in,
        scales,
        row_router,
        routers,
        load_sem,
        send_sem,
        recv_sem,
        first_send,
        first_recv,
        batch_send,
        batch_recv,
        row_send,
        row_recv,
        bank_send,
        bank_recv,
        late_sem,
    ) = refs[parts:]
    experts, rows, columns = gate_ref.shape
    width = columns // parts
    total = 2 * experts
    batches = total // parts
    half = parts // 2
    depth = ring.shape[0]
    sent = total - late[0].shape[0]
    bits = parts.bit_length() - 1
    me, bank = lax.axis_index("zero"), lax.axis_index("bank")
    side, place = lax.rem(me, 2), lax.div(me, 2)
    masks = sorted(range(1, parts), key=lambda m: (m == 1, m % 2, -(m // 2)))
    peers = [flip(me, mask, bits) for mask in masks]
    partner = flip(me, 1, bits)
    cohort = [flip(me, mask, bits) for mask in masks if mask % 2 == 0]
    own_rows = pl.ds(pl.multiple_of(me * rows, 128), rows)

    def remote(src, dst, send, recv, **device):
        return pltpu.make_async_remote_copy(
            src_ref=src,
            dst_ref=dst,
            send_sem=send,
            recv_sem=recv,
            device_id=device,
            device_id_type=MESH,
        )

    def load(e):
        slot = lax.rem(e, depth)

        @pl.when(e < experts)
        def _():
            pltpu.make_async_copy(gate_ref.at[e], ring.at[slot], load_sem.at[slot]).start()

        @pl.when(e >= experts)
        def _():
            pltpu.make_async_copy(
                up_ref.at[e - experts], ring.at[slot], load_sem.at[slot]
            ).start()

    def square(e):
        slot = lax.rem(e, depth)
        pltpu.make_async_copy(gate_ref.at[0], ring.at[slot], load_sem.at[slot]).wait()
        w = ring[slot]
        return jnp.sum(w * w, axis=0, keepdims=True)

    def where_of(e):
        i = lax.rem(e, parts)
        return lax.div(e, parts), lax.rem(i, 2), lax.div(i, 2)

    def first_square(e, carry):
        first_in[me, e] = square(e)
        load(e + LOADS)
        return carry

    def later_square(e, carry):
        sums[where_of(e)] = square(e)
        return carry

    groups = ((0, FIRST), (FIRST, parts - FIRST))

    def send_first(group):
        part = first_in.at[me, pl.ds(*groups[group])]
        for peer in peers:
            remote(part, part, first_send.at[group], first_recv.at[group], zero=peer).start()

    def all_first(group):
        part = first_in.at[pl.ds(0, parts - 1), pl.ds(*groups[group])]
        return remote(part, part, first_send.at[group], first_recv.at[group], zero=me)

    def finish_first(group):
        all_first(group).wait_recv()
        for e in range(groups[group][0], sum(groups[group])):
            whole = first_in[0, e]
            for part in range(1, parts):
                whole = whole + first_in[part, e]
            scales[0, e % 2, e // 2] = jnp.sqrt(whole)

    def pair_sums(b):
        return remote(
            sums.at[b, 1 - side],
            pair_in.at[b],
            batch_send.at[0, b],
            batch_recv.at[0, b],
            zero=partner,
        )

    def chip_piece(b, peer):
        return remote(
            chip_sums.at[b, lax.div(peer, 2)],
            chip_in.at[b, place],
            batch_send.at[1, b],
            batch_recv.at[1, b],
            zero=peer,
        )

    def scale_piece(b, peer):
        row = scales.at[b, side, place]
        return remote(row, row, batch_send.at[2, b], batch_recv.at[2, b], zero=peer)

    def pair_scales(b):
        mine = scales.at[b, side]
        return remote(mine, mine, batch_send.at[3, b], batch_recv.at[3, b], zero=partner)

    def all_pieces(stage, b):
        part = chip_in.at[b, pl.ds(0, half - 1)]
        return remote(part, part, batch_send.at[stage, b], batch_recv.at[stage, b], zero=me)

    def stage_chip(b):
        pair_sums(b).wait_recv()
        for q in range(half):
            chip_sums[b, q] = pair_in[b, q] + sums[b, side, q]
        chip_in[b, place] = chip_sums[b, place]
        for peer in cohort:
            chip_piece(b, peer).start()

    def stage_scale(b):
        all_pieces(1, b).wait_recv()
        whole = chip_in[b, 0]
        for q in range(1, half):
            whole = whole + chip_in[b, q]
        scales[b, side, place] = jnp.sqrt(whole)
        for peer in cohort:
            scale_piece(b, peer).start()

    def stage_share(b):
        all_pieces(2, b).wait_recv()
        pair_scales(b).start()

    def keep_scales(b):
        start = pl.multiple_of(b * parts, 8)
        whole = jnp.concatenate([scales[b, j % 2, j // 2] for j in range(parts)], axis=0)
        own = jnp.zeros((parts, width), jnp.float32)
        for part in range(parts):
            own = jnp.where(me == part, whole[:, part * width : (part + 1) * width], own)
        scale_out[pl.ds(start, parts), :] = own

    def send_piece(e, slot, at):
        return remote(
            outgoing.at[slot, peers[at]],
            landing.at[e, :, own_rows],
            send_sem.at[slot, at],
            recv_sem.at[me],
            zero=peers[at],
        )

    def late_copies(slot, at):
        for mask in range(parts):
            yield pltpu.make_async_copy(
                outgoing.at[slot, flip(me, mask, bits)],
                late[mask].at[at],
                late_sem.at[at, mask],
            )

    def row_piece(peer):
        return remote(
            row_router, routers.at[bank, :, own_rows], row_send, row_recv, zero=peer
        )

    def all_rows():
        part = routers.at[bank, :, pl.ds(0, (parts - 1) * rows)]
        return remote(part, part, row_send, row_recv, zero=me)

    def line(hop, send):
        for way, turn in enumerate((1, -1)):
            source = bank - turn * (hop - 1 if send else hop)
            target = bank + turn
            fits = jnp.logical_and(source >= 0, source < banks)
            if send:
                fits = fits & jnp.logical_and(target >= 0, target < banks)
            yield fits, source, target, (way, hop)

    def line_copy(source, target, at):
        part = routers.at[source]
        return remote(part, part, bank_send.at[at], bank_recv.at[at], bank=target)

    def line_start(hop):
        for fits, source, target, at in line(hop, True):

            @pl.when(fits)
            def _():
                line_copy(source, target, at).start()

    def line_arrived(hop):
        for fits, source, target, at in line(hop, False):

            @pl.when(fits)
            def _():
                line_copy(source, bank, at).wait_recv()

    def line_left(hop):
        for fits, source, target, at in line(hop, True):

            @pl.when(fits)
            def _():
                line_copy(source, target, at).wait_send()

    for e in range(LOADS):
        load(jnp.int32(e))

    barrier = pltpu.get_barrier_semaphore()
    for peer in peers:
        pl.semaphore_signal(barrier, inc=1, device_id={"zero": peer}, device_id_type=MESH)
    around = jnp.int32(0)
    for other in (bank - 1, bank + 1):
        fits = jnp.logical_and(other >= 0, other < banks)
        around = around + jnp.where(fits, 1, 0)

        @pl.when(fits)
        def _():
            pl.semaphore_signal(
                barrier, inc=1, device_id={"bank": other}, device_id_type=MESH
            )

    part_router = (router_ref[...] * gain_ref[...]).astype(jnp.bfloat16)
    row_router[...] = part_router
    routers[bank, :, own_rows] = part_router
    lax.fori_loop(0, FIRST, first_square, 0)
    pl.semaphore_wait(barrier, parts - 1 + around)
    send_first(0)
    for peer in peers:
        row_piece(peer).start()
    lax.fori_loop(FIRST, parts, first_square, 0)
    send_first(1)
    finish_first(0)

    def step(s, carry):
        b, i = lax.div(s, parts), lax.rem(s, parts)
        slot = lax.rem(s, SLOTS)

        @pl.when(jnp.logical_and(i == 0, b > 0))
        def _():
            pair_scales(b).wait_recv()

        @pl.when(s >= SLOTS)
        def _():
            for at in range(parts - 1):
                send_piece(s, slot, at).wait_send()

        turned = (ring[lax.rem(s, depth)] / scales[where_of(s)]).T
        for part in range(parts):
            outgoing[slot, part] = turned[part * width : (part + 1) * width].astype(
                jnp.bfloat16
            )

        @pl.when(s < sent)
        def _():
            landing[s, :, own_rows] = outgoing[slot, me]

        @pl.when(s + 2 * parts + LOADS < total)
        def _():
            load(s + 2 * parts + LOADS)

        @pl.when(s < sent)
        def _():
            for at in range(parts - 1):
                send_piece(s, slot, at).start()

        @pl.when(s >= sent)
        def _():
            for copy in late_copies(slot, s - sent):
                copy.start()

        @pl.when(s == 0)
        def _():
            def ahead(e, carry):
                load(e + LOADS)
                return later_square(e, carry)

            lax.fori_loop(parts, 2 * parts, ahead, 0)
            pair_sums(1).start()

        @pl.when(s == 1)
        def _():
            finish_first(1)

        @pl.when(s + 2 * parts < total)
        def _():
            later_square(s + 2 * parts, 0)

        @pl.when(jnp.logical_and(i == parts - 1, b + 2 < batches))
        def _():
            pair_sums(b + 2).start()

        @pl.when(b + 1 < batches)
        def _():
            @pl.when(i == 1)
            def _():
                stage_chip(b + 1)

            @pl.when(i == 3)
            def _():
                stage_scale(b + 1)

            @pl.when(i == 5)
            def _():
                stage_share(b + 1)

        @pl.when(i == 2)
        def _():
            keep_scales(b)

        for hop in range(1, banks):

            @pl.when(s == hop * parts)
            def _():
                if hop == 1:
                    all_rows().wait_recv()
                else:
                    line_arrived(hop - 1)
                line_start(hop)

        return carry

    lax.fori_loop(0, total, step, 0)

    line_arrived(banks - 1)
    for hop in range(1, banks):
        line_left(hop)
    all_rows().wait_send()
    turned = routers[...].reshape(banks * router_ref.shape[0], parts * rows).T
    router_out[...] = turned

    for group in range(2):
        all_first(group).wait_send()
    for b in range(1, batches):
        pair_sums(b).wait_send()
        all_pieces(1, b).wait_send()
        all_pieces(2, b).wait_send()
        pair_scales(b).wait_send()
    for at in range(total - sent):
        for copy in late_copies((sent + at) % SLOTS, at):
            copy.wait()
    for s in range(total - SLOTS, sent):
        for at in range(parts - 1):
            send_piece(s, s % SLOTS, at).wait_send()
    for peer in peers:
        region = landing.at[pl.ds(0, sent), :, pl.ds(pl.multiple_of(peer * rows, 128), rows)]
        remote(region, region, recv_sem.at[me], recv_sem.at[peer], zero=me).wait_recv()


def exchange(parts, banks, w_gate, w_up, router_weight, router_gain):
    experts, rows, columns = w_gate.shape
    width = columns // parts
    total = 2 * experts
    batches = total // parts
    held = router_weight.shape[1]
    vmem = pl.BlockSpec(memory_space=pltpu.VMEM)
    hbm = pl.BlockSpec(memory_space=pl.ANY)
    depth = 3 * parts
    half = parts // 2
    row = (1, columns)
    dma = pltpu.SemaphoreType.DMA
    return pl.pallas_call(
        functools.partial(exchange_kernel, parts, banks),
        in_specs=[hbm, hbm, vmem, vmem],
        out_specs=[vmem] * 3 + [hbm] * parts,
        out_shape=[
            pltpu.VMEM((total, width, parts * rows), jnp.bfloat16),
            pltpu.VMEM((total, width), jnp.float32),
            pltpu.VMEM((parts * rows, banks * held), jnp.bfloat16),
        ]
        + [pltpu.HBM((LATE, width, rows), jnp.bfloat16)] * parts,
        scratch_shapes=[
            pltpu.VMEM((depth, rows, columns), jnp.float32),
            pltpu.VMEM((SLOTS, parts, width, rows), jnp.bfloat16),
            pltpu.VMEM((parts, parts) + row, jnp.float32),
            pltpu.VMEM((batches, 2, half) + row, jnp.float32),
            pltpu.VMEM((batches, half) + row, jnp.float32),
            pltpu.VMEM((batches, half) + row, jnp.float32),
            pltpu.VMEM((batches, half) + row, jnp.float32),
            pltpu.VMEM((batches, 2, half) + row, jnp.float32),
            pltpu.VMEM((held, rows), jnp.bfloat16),
            pltpu.VMEM((banks, held, parts * rows), jnp.bfloat16),
            dma((depth,)),
            dma((SLOTS, parts - 1)),
            dma((parts,)),
            dma((2,)),
            dma((2,)),
            dma((4, batches)),
            dma((4, batches)),
            dma,
            dma,
            dma((2, banks)),
            dma((2, banks)),
            dma((LATE, parts)),
        ],
        cost_estimate=pl.CostEstimate(
            flops=total * rows * columns * 60,
            bytes_accessed=total * rows * columns * 4,
            transcendentals=0,
        ),
        compiler_params=pltpu.CompilerParams(
            collective_id=0, has_side_effects=True, vmem_limit_bytes=VMEM_LIMIT
        ),
        name="exchange",
    )(
        pltpu.with_memory_space_constraint(w_gate, pltpu.HBM),
        pltpu.with_memory_space_constraint(w_up, pltpu.HBM),
        router_weight.T,
        router_gain[None, :],
    )


def deliver_kernel(pieces, landing, scales, router, gate, up, scale_gate, scale_up, out, sem):
    experts = gate.shape[0]
    size = experts // pieces
    copies = []
    for which, target in enumerate((gate, up)):
        for piece in range(pieces):
            first = piece * size
            count = min(size, experts - which * LATE - first)
            if count > 0:
                copies.append(
                    (
                        landing.at[pl.ds(which * experts + first, count)],
                        target.at[pl.ds(first, count)],
                    )
                )
    copies.append((scales.at[pl.ds(0, experts)], scale_gate))
    copies.append((scales.at[pl.ds(experts, experts)], scale_up))
    copies.append((router, out))
    handles = [
        pltpu.make_async_copy(source, target, sem.at[at])
        for at, (source, target) in enumerate(copies)
    ]
    for handle in handles:
        handle.start()
    for handle in handles:
        handle.wait()


def in_vmem(*arrays):
    return [pltpu.with_memory_space_constraint(x, pltpu.VMEM) for x in arrays]


def deliver(landing, scales, router):
    total, width, rows = landing.shape
    experts = total // 2
    pieces = 8 if experts % 8 == 0 else 1
    vmem = pl.BlockSpec(memory_space=pltpu.VMEM)
    hbm = pl.BlockSpec(memory_space=pl.ANY)
    return pl.pallas_call(
        functools.partial(deliver_kernel, pieces),
        in_specs=[vmem] * 3,
        out_specs=[hbm] * 5,
        out_shape=[
            jax.ShapeDtypeStruct((experts, width, rows), landing.dtype),
            jax.ShapeDtypeStruct((experts, width, rows), landing.dtype),
            jax.ShapeDtypeStruct((experts, width), jnp.float32),
            jax.ShapeDtypeStruct((experts, width), jnp.float32),
            jax.ShapeDtypeStruct(router.shape, router.dtype),
        ],
        scratch_shapes=[pltpu.SemaphoreType.DMA((2 * pieces + 3,))],
        cost_estimate=pl.CostEstimate(
            flops=total * rows * width, bytes_accessed=4 * total * rows * width, transcendentals=0
        ),
        compiler_params=pltpu.CompilerParams(vmem_limit_bytes=2**20),
        name="deliver",
    )(*in_vmem(landing, scales, router))


def finish_kernel(parts, *refs):
    blocks, up, sem = refs[:parts], refs[-2], refs[-1]
    count, _, rows = blocks[0].shape
    bits = parts.bit_length() - 1
    me = lax.axis_index("zero")
    first = up.shape[0] - count
    handles = []
    for mask, block in enumerate(blocks):
        source = flip(me, mask, bits)
        columns = pl.ds(pl.multiple_of(source * rows, 128), rows)
        handles.append(
            pltpu.make_async_copy(block, up.at[pl.ds(first, count), :, columns], sem.at[mask])
        )
    for handle in handles:
        handle.start()
    for handle in handles:
        handle.wait()


def finish(blocks, up):
    vmem = pl.BlockSpec(memory_space=pltpu.VMEM)
    hbm = pl.BlockSpec(memory_space=pl.ANY)
    parts = len(blocks)
    return pl.pallas_call(
        functools.partial(finish_kernel, parts),
        in_specs=[vmem] * parts + [hbm],
        out_specs=hbm,
        out_shape=jax.ShapeDtypeStruct(up.shape, up.dtype),
        input_output_aliases={parts: 0},
        scratch_shapes=[pltpu.SemaphoreType.DMA((parts,))],
        cost_estimate=pl.CostEstimate(flops=10**6, bytes_accessed=10**6, transcendentals=0),
        compiler_params=pltpu.CompilerParams(vmem_limit_bytes=4 * 2**20),
        name="finish",
    )(*blocks, up)


def shards_blocked(parts, banks, w_gate, w_up, router_weight, router_gain):
    landing, scales, router, *late = exchange(
        parts, banks, w_gate, w_up, router_weight, router_gain
    )
    blocks = list(late)
    for mask in sorted(range(1, parts), key=lambda m: (m == 1, m % 2, -(m // 2))):
        pairs = [(i, i ^ mask) for i in range(parts)]
        blocks[mask] = lax.ppermute(late[mask], "zero", pairs)
    gate, up, scale_gate, scale_up, router = deliver(landing, scales, router)
    up = finish(blocks, up)
    return gate.transpose(0, 2, 1), up.transpose(0, 2, 1), scale_gate, scale_up, router


def shards_plain(w_gate, w_up, router_weight, router_gain):
    total_gate, total_up = lax.psum(
        (jnp.sum(w_gate * w_gate, axis=1), jnp.sum(w_up * w_up, axis=1)), "zero"
    )
    results, own = [], []
    for w, total in ((w_gate, total_gate), (w_up, total_up)):
        scale = jnp.sqrt(total)
        narrow = (w / jnp.expand_dims(scale, 1)).astype(jnp.bfloat16)
        serve = lax.all_to_all(narrow, "zero", split_axis=2, concat_axis=1, tiled=True)
        width = serve.shape[2]
        results.append(serve)
        own.append(
            lax.dynamic_slice_in_dim(scale, lax.axis_index("zero") * width, width, axis=1)
        )
    part_router = (router_weight * router_gain[:, None]).astype(jnp.bfloat16)
    row_router = lax.all_gather(part_router, "zero", axis=0, tiled=True)
    serve_router = lax.all_gather(row_router, "bank", axis=1, tiled=True)
    return (*results, *own, serve_router)


def solution(mesh):
    parts, banks = mesh.shape["zero"], mesh.shape["bank"]
    placed = (P("bank", "zero", None), P("bank", "zero", None), P("zero", "bank"), P("zero"))

    def shards(w_gate, w_up, router_weight, router_gain):
        experts, rows, columns = w_gate.shape
        held = router_weight.shape[1]
        total = 2 * experts
        power = parts & (parts - 1) == 0 and parts % 8 == 0
        whole = rows % 128 == 0 and columns % (16 * parts) == 0 and held % 16 == 0
        if power and whole and total % parts == 0 and total >= max(3, banks) * parts:
            return shards_blocked(parts, banks, w_gate, w_up, router_weight, router_gain)
        return shards_plain(w_gate, w_up, router_weight, router_gain)

    return jax.shard_map(
        shards,
        mesh=mesh,
        in_specs=placed,
        out_specs=(
            P("bank", None, "zero"),
            P("bank", None, "zero"),
            P("bank", "zero"),
            P("bank", "zero"),
            P(),
        ),
        check_vma=False,
    )
```
